32 devices in a mesh: row: 4 (over y, core), col: 8 (over z, x).
Axes of the slice: x: 2, y: 2, z: 4, core: 2. Of those that a mesh axis runs over, the one named last changes fastest.
Arguments:
- obs_cell: int32 [32, 16, 32, 128], P(('row', 'col')), may hold values from 0 to 8388607, as said below
- obs_value: bfloat16 [32, 16, 32, 128], P(('row', 'col')), may hold values from -6 to 6
- obs_weight: bfloat16 [32, 16, 32, 128], P(('row', 'col')), may hold values from 0.5 to 2
- obs_count: int32 [32, 16, 32], P(('row', 'col')), may hold values from 0 to 128, as said below
- kappa_field: float32 [2048, 4096], P('row', 'col'), may hold values from 0.2 to 6
Outputs:
- solution_field: float32 [2048, 4096], P('row', 'col')
- residual: float32 [2048, 4096], P('row', 'col')
The draws below stay inside these ranges and needn't reach their ends.
Inputs may be any that keep to these rules, and one draw needn't show every extreme that they name: `obs_cell`: block (s, t, d) holds observations for tile t of device d, where device d is number d // 8 along row and d % (8) along col, and tile t is number t // 4 among the device's tiles along rows and t % (4) along columns, each tile 128 by 128 cells; every slot of the block, padding included, names a cell of that tile as row * 4096 + column. Slots at positions obs_count and beyond are padding. For one owner device, chosen afresh in each draw, every block from every source and tile is full.
All inputs are finite; a program needn't handle non-finite values.
Results may differ from the reference program's by a relative error of at most 0.0029.
Values may be sent and summed in bfloat16 or wider, within the bound.
A program may use at most 64 MiB of HBM per device.

```python
import math
import jax
import jax.numpy as jnp
from jax import lax

CR = 512
CC = 512
TILE = 128
BLOCK = 128
ITERS = 3
TILES = 16
NR = 2048
NC = 4096
DEVICES = 32


def draw_obs_count(key, part):
    key_pop, key_hot, key_load = jax.random.split(jax.random.fold_in(key, 11), 3)
    owners = jnp.arange(DEVICES, dtype=jnp.int32)
    popular = jax.random.randint(key_pop, (DEVICES,), 1, 5, dtype=jnp.int32)
    hottest = jax.random.randint(key_hot, (), 0, DEVICES, dtype=jnp.int32)
    popular = jnp.where(owners == hottest, 8, popular)
    raw_load = jax.random.randint(key_load, (DEVICES, TILES, DEVICES), 0, 2 * BLOCK + 1, dtype=jnp.int32)
    counts = jnp.minimum(BLOCK, raw_load * popular[None, None, :] // 4)
    counts = jnp.where(owners[None, None, :] == hottest, BLOCK, counts)
    return counts.astype(jnp.int32)


def draw_obs_cell(key, part):
    key_row, key_col = jax.random.split(jax.random.fold_in(key, 23))
    full_shape = (DEVICES, TILES, DEVICES, BLOCK)
    local_row = jax.random.randint(key_row, full_shape, 0, TILE, dtype=jnp.int32)
    local_col = jax.random.randint(key_col, full_shape, 0, TILE, dtype=jnp.int32)
    owners = jnp.arange(DEVICES, dtype=jnp.int32)[None, None, :, None]
    tile_ids = jnp.arange(TILES, dtype=jnp.int32)[None, :, None, None]
    grid_cols = NC // CC
    tile_span = CC // TILE
    lattice_row = owners // grid_cols * CR + tile_ids // tile_span * TILE + local_row
    lattice_col = owners % grid_cols * CC + tile_ids % tile_span * TILE + local_col
    return (lattice_row * NC + lattice_col).astype(jnp.int32)


def steps_of(own_key, extent, pieces, smallest, largest):
    def one(axis_at, shards_of):
        steps = jax.random.uniform(jax.random.fold_in(jax.random.fold_in(own_key, 6), axis_at), (shards_of,), jnp.float32, smallest / len(pieces), largest / len(pieces))
        return jnp.repeat(jnp.exp(steps), extent[axis_at] // shards_of).reshape((-1,) + (1,) * (len(extent) - axis_at - 1))

    gain = one(*pieces[0])
    for cut in pieces[1:]:
        gain = gain * one(*cut)
    return gain


def normal_values(key, extent, width, limit, cuts=(), held_as=jnp.bfloat16):
    array = jax.random.normal(key, extent, jnp.float32) * width
    if len(cuts) > 0:
        array = steps_of(key, extent, cuts, -0.22, 0.18) * array
    return jnp.clip(array, min=-limit, max=limit).astype(held_as)


def setup_inputs(seed: int = 0) -> dict:
    key_of = jax.random.split(jax.random.key(seed), 6)
    obs_cell = draw_obs_cell(jax.random.fold_in(key_of[5], 71), 0)
    obs_value = normal_values(key_of[1], (DEVICES, TILES, DEVICES, BLOCK), 1.0, 6.0, ((0, 32),))
    obs_weight = jnp.clip(jnp.exp(math.log(2.0) - 1.3862944 * jax.random.uniform(key_of[2], (DEVICES, TILES, DEVICES, BLOCK), jnp.float32) ** steps_of(key_of[2], (DEVICES, TILES, DEVICES, BLOCK), ((0, 32),), -0.2, 0.2)), 0.5, 2.0).astype(jnp.bfloat16)
    obs_count = draw_obs_count(jax.random.fold_in(key_of[5], 71), 0)
    kappa_field = jnp.clip(jnp.exp(math.log(6.0) - 3.4011974 * jax.random.uniform(key_of[4], (NR, NC), jnp.float32) ** steps_of(key_of[4], (NR, NC), ((0, 4), (1, 8)), -0.2, 0.2)), 0.2, 6.0)
    return {"obs_cell": obs_cell, "obs_value": obs_value, "obs_weight": obs_weight, "obs_count": obs_count, "kappa_field": kappa_field}


smooth_weight = 0.05


def stencil_step(field, kappa_field):
    padded = jnp.pad(field, 1)
    beside = padded[2:, 1:-1] + padded[:-2, 1:-1]
    beside = beside + padded[1:-1, 2:] + padded[1:-1, :-2]
    return (4.0 + kappa_field) * field - beside


def reference(obs_cell, obs_value, obs_weight, obs_count, kappa_field):
    rows_all, cols_all = kappa_field.shape
    positions = jnp.arange(BLOCK, dtype=jnp.int32)
    is_live = positions < obs_count[..., None]
    weight_wide = obs_weight.astype(jnp.float32)
    product = (weight_wide * obs_value.astype(jnp.float32)).astype(jnp.bfloat16)
    product = lax.optimization_barrier(product)
    masked_weight = jnp.where(is_live, weight_wide, jnp.float32(0.0)).reshape(-1)
    masked_resp = jnp.where(is_live, product.astype(jnp.float32), jnp.float32(0.0)).reshape(-1)
    flat_cells = obs_cell.reshape(-1).astype(jnp.int32)
    empty = jnp.zeros((rows_all * cols_all,), jnp.float32)
    weight_field = empty.at[flat_cells].add(masked_weight).reshape(rows_all, cols_all)
    response = empty.at[flat_cells].add(masked_resp).reshape(rows_all, cols_all)

    def operate(field):
        inner = stencil_step(field, kappa_field)
        return weight_field * field + smooth_weight * stencil_step(inner, kappa_field)

    solution_field = jnp.zeros_like(response)
    residual, direction = response, response
    norm_now = jnp.sum(residual * residual)
    for step in range(ITERS):
        image = operate(direction)
        alpha = norm_now / jnp.sum(direction * image)
        solution_field = solution_field + alpha * direction
        residual = residual - alpha * image
        norm_next = jnp.sum(residual * residual)
        direction = residual + (norm_next / norm_now) * direction
        norm_now = norm_next
    return solution_field, residual
```

```python
import functools

import jax
import jax.numpy as jnp
from jax import lax
from jax.experimental import pallas as pl
from jax.experimental.pallas import tpu as pltpu
from jax.sharding import PartitionSpec as P

TILE = 128
ITERS = 3
HALO = 8
PAD = 2 * HALO
STRIP = 24
CHUNK = 1024

smooth_weight = 0.05

MESH = pl.DeviceIdType.MESH


def greet_all(me, count, cols):
    barrier = pltpu.get_barrier_semaphore()

    def signal(k, carry):
        peer = lax.rem(me + k, count)
        pl.semaphore_signal(
            barrier, inc=1, device_id=(peer // cols, lax.rem(peer, cols)), device_id_type=MESH
        )
        return carry

    lax.fori_loop(1, count, signal, 0)
    pl.semaphore_wait(barrier, count - 1)


def exchange_kernel(rows, cols, code_ref, pair_ref, code_out, pair_out, send_sems, recv_sems, own_sems):
    count = rows * cols
    me = lax.axis_index("row") * cols + lax.axis_index("col")
    own_code = pltpu.make_async_copy(code_ref.at[me], code_out.at[me], own_sems.at[0])
    own_pair = pltpu.make_async_copy(pair_ref.at[me], pair_out.at[me], own_sems.at[1])
    own_code.start()
    own_pair.start()
    greet_all(me, count, cols)

    def copies(k):
        peer = lax.rem(me + k, count)
        where = (peer // cols, lax.rem(peer, cols))
        return [
            pltpu.make_async_remote_copy(
                src_ref=src.at[peer],
                dst_ref=dst.at[me],
                send_sem=send_sems.at[which, k],
                recv_sem=recv_sems.at[which, k],
                device_id=where,
                device_id_type=MESH,
            )
            for which, (src, dst) in enumerate(((code_ref, code_out), (pair_ref, pair_out)))
        ]

    def begin(k, carry):
        for copy in copies(k):
            copy.start()
        return carry

    def finish(k, carry):
        source = lax.rem(me + count - k, count)
        for which, (src, dst) in enumerate(((code_ref, code_out), (pair_ref, pair_out))):
            pltpu.make_async_remote_copy(
                src_ref=src.at[source],
                dst_ref=dst.at[source],
                send_sem=send_sems.at[which, k],
                recv_sem=recv_sems.at[which, k],
                device_id=(source // cols, lax.rem(source, cols)),
                device_id_type=MESH,
            ).wait()
        return carry

    lax.fori_loop(1, count, begin, 0)
    lax.fori_loop(1, count, finish, 0)
    own_code.wait()
    own_pair.wait()


def bin_kernel(members_ref, weight_ref, response_ref):
    slots = members_ref.shape[2]
    chunk = min(CHUNK, slots)
    offsets = (
        lax.broadcasted_iota(jnp.int32, (TILE, chunk), 0).astype(jnp.float32).astype(jnp.bfloat16)
    )
    one = jnp.ones((TILE, chunk), jnp.bfloat16)
    zero = jnp.zeros((TILE, chunk), jnp.bfloat16)

    def part(at, total):
        def spread(which):
            piece = members_ref[0, which : which + 1, pl.ds(pl.multiple_of(at * chunk, chunk), chunk)]
            return jnp.broadcast_to(piece.astype(jnp.bfloat16), (TILE, chunk))

        row_hot = jnp.where(spread(0) == offsets, one, zero)
        col_hit = spread(1) == offsets
        stacked = jnp.concatenate(
            [jnp.where(col_hit, spread(2), zero), jnp.where(col_hit, spread(3), zero)], axis=0
        )
        return total + lax.dot_general(
            row_hot, stacked, (((1,), (1,)), ((), ())), preferred_element_type=jnp.float32
        )

    total = lax.fori_loop(
        0, slots // chunk, part, jnp.zeros((TILE, 2 * TILE), jnp.float32)
    )
    weight_ref[...] = total[:, :TILE]
    response_ref[...] = total[:, TILE:]


def smooth_kernel(
    rows, cols, b_ref, w_ref, k_ref, x_ref, r_ref,
    res, wgt, kap, live, inner, image, along, course,
    send_low, send_high, recv_low, recv_high, mine, sums,
    row_send, row_recv, col_send, col_recv, sum_send, sum_recv,
):
    count = rows * cols
    my_row, my_col = lax.axis_index("row"), lax.axis_index("col")
    me = my_row * cols + my_col
    height, width = b_ref.shape
    full = width + 128
    own = pl.ds(PAD, height)
    fields = ((b_ref, res), (w_ref, wgt), (k_ref, kap))
    tall = res.shape[0]

    for _, field in fields:
        field[0:PAD, :] = jnp.zeros((PAD, full), jnp.float32)
        field[PAD + height :, :] = jnp.zeros((tall - PAD - height, full), jnp.float32)
    inner[0:HALO, :] = jnp.zeros((HALO, full), jnp.float32)
    inner[PAD + height + HALO : 2 * PAD + height, :] = jnp.zeros((HALO, full), jnp.float32)
    recv_low[...] = jnp.zeros_like(recv_low)
    recv_high[...] = jnp.zeros_like(recv_high)
    greet_all(me, count, cols)

    up, down = my_row > 0, my_row < rows - 1
    left, right = my_col > 0, my_col < cols - 1

    def row_copies(way):
        made = []
        for at, (src, dst) in enumerate(fields):
            if way == 0:
                source, target = src.at[pl.ds(0, HALO), :], dst.at[pl.ds(PAD + height, HALO), pl.ds(0, width)]
                where = (my_row - 1, my_col)
            else:
                source, target = src.at[pl.ds(height - HALO, HALO), :], dst.at[pl.ds(HALO, HALO), pl.ds(0, width)]
                where = (my_row + 1, my_col)
            made.append(
                pltpu.make_async_remote_copy(
                    src_ref=source, dst_ref=target,
                    send_sem=row_send.at[way, at], recv_sem=row_recv.at[way, at],
                    device_id=where, device_id_type=MESH,
                )
            )
        return made

    def col_copy(way):
        source, target, where = (
            (send_low, recv_high, (my_row, my_col - 1)),
            (send_high, recv_low, (my_row, my_col + 1)),
        )[way]
        return pltpu.make_async_remote_copy(
            src_ref=source, dst_ref=target, send_sem=col_send.at[way], recv_sem=col_recv.at[way],
            device_id=where, device_id_type=MESH,
        )

    for way, there in ((0, up), (1, down)):

        @pl.when(there)
        def _(way=way):
            for copy in row_copies(way):
                copy.start()

    def fill(i, carry):
        at = pl.multiple_of(i * 32, 32)
        for src, dst in fields:
            dst[pl.ds(PAD + at, 32), 0:width] = src[pl.ds(at, 32), :]
        return carry

    lax.fori_loop(0, height // 32, fill, 0)

    for way, there in ((0, up), (1, down)):

        @pl.when(there)
        def _(way=way):
            for copy in row_copies(way):
                copy.wait_send()

        @pl.when((down, up)[way])
        def _(way=way):
            for copy in row_copies(way):
                copy.wait_recv()

    def pack(i, carry):
        at = pl.multiple_of(i * 128, 128)
        for which, (_, field) in enumerate(fields):
            low = field[pl.ds(at, 128), 0:128].T
            send_low[which * HALO : (which + 1) * HALO, pl.ds(at, 128)] = low[:HALO]
            high = field[pl.ds(at, 128), width - 128 : width].T
            send_high[which * HALO : (which + 1) * HALO, pl.ds(at, 128)] = high[128 - HALO :]
        return carry

    lax.fori_loop(0, tall // 128, pack, 0)
    for way, there in ((0, left), (1, right)):

        @pl.when(there)
        def _(way=way):
            col_copy(way).start()

    for way, there in ((0, left), (1, right)):

        @pl.when(there)
        def _(way=way):
            col_copy(way).wait_send()

        @pl.when((right, left)[way])
        def _(way=way):
            col_copy(way).wait_recv()

    gap = jnp.zeros((128 - 2 * HALO, 128), jnp.float32)

    def unpack(i, carry):
        at = pl.multiple_of(i * 128, 128)
        for which, (_, field) in enumerate(fields):
            part = slice(which * HALO, (which + 1) * HALO)
            both = jnp.concatenate(
                [recv_high[part, pl.ds(at, 128)], gap, recv_low[part, pl.ds(at, 128)]], axis=0
            )
            field[pl.ds(at, 128), width:full] = both.T
        return carry

    lax.fori_loop(0, tall // 128, unpack, 0)

    strips = (height + 2 * HALO) // STRIP
    top = jnp.where(up, HALO, PAD)
    bottom = PAD + height + jnp.where(down, HALO, 0)
    high_end = width + jnp.where(right, HALO, 0)
    low_begin = full - jnp.where(left, HALO, 0)

    def start_of(i):
        return pl.multiple_of(HALO + i * STRIP, 8)

    def prepare(i, carry):
        at = start_of(i)
        row = lax.broadcasted_iota(jnp.int32, (STRIP, full), 0) + at
        col = lax.broadcasted_iota(jnp.int32, (STRIP, full), 1)
        inside = (row >= top) & (row < bottom) & ((col < high_end) | (col >= low_begin))
        mask = jnp.where(inside, 1.0, 0.0).astype(jnp.float32)
        live[pl.ds(at, STRIP), :] = mask
        kap[pl.ds(at, STRIP), :] = jnp.where(inside, 4.0 + kap[pl.ds(at, STRIP), :], 0.0)
        return carry

    lax.fori_loop(0, strips, prepare, 0)

    def stencil(field, at):
        slab = field[pl.ds(pl.multiple_of(at - HALO, 8), STRIP + 2 * HALO), :]
        center = slab[HALO : HALO + STRIP]
        beside = slab[HALO + 1 : HALO + 1 + STRIP] + slab[HALO - 1 : HALO - 1 + STRIP]
        beside = beside + pltpu.roll(center, full - 1, axis=1) + pltpu.roll(center, 1, axis=1)
        here = pl.ds(at, STRIP)
        return kap[here, :] * center - live[here, :] * beside

    def operate():
        def first(i, carry):
            at = start_of(i)
            inner[pl.ds(at, STRIP), :] = stencil(res, at)
            return carry

        def second(i, carry):
            at = start_of(i)
            here = pl.ds(at, STRIP)
            image[here, :] = wgt[here, :] * res[here, :] + smooth_weight * stencil(inner, at)
            return carry

        lax.fori_loop(0, strips, first, 0)
        lax.fori_loop(0, strips, second, 0)

    lane = lax.broadcasted_iota(jnp.int32, (1, 128), 1)

    def two_products(step):
        def add(i, carry):
            norm, curve = carry
            here = pl.ds(pl.multiple_of(PAD + i * 16, 8), 16)
            a, c = res[here, 0:width], image[here, 0:width]
            aa, ac = a * a, a * c
            return norm + (aa[:8] + aa[8:]), curve + (ac[:8] + ac[8:])

        zero = jnp.zeros((8, width), jnp.float32)
        norm, curve = lax.fori_loop(0, height // 16, add, (zero, zero))
        norm = jnp.sum(jnp.sum(norm, axis=0, keepdims=True), axis=1, keepdims=True)
        curve = jnp.sum(jnp.sum(curve, axis=0, keepdims=True), axis=1, keepdims=True)
        both = jnp.where(lane == 0, norm, jnp.where(lane == 1, curve, 0.0))
        mine[step] = both
        sums[step, me] = both

        def copy_to(k, peer, slot):
            return pltpu.make_async_remote_copy(
                src_ref=mine.at[step], dst_ref=sums.at[step, slot],
                send_sem=sum_send.at[step, k], recv_sem=sum_recv.at[step, k],
                device_id=(peer // cols, lax.rem(peer, cols)), device_id_type=MESH,
            )

        def begin(k, carry):
            copy_to(k, lax.rem(me + k, count), me).start()
            return carry

        def finish(k, carry):
            source = lax.rem(me + count - k, count)
            copy_to(k, source, source).wait()
            return carry

        lax.fori_loop(1, count, begin, 0)
        lax.fori_loop(1, count, finish, 0)
        total = jnp.sum(sums[step], axis=0)
        norm = jnp.sum(jnp.where(lane == 0, total, 0.0), axis=1, keepdims=True)
        curve = jnp.sum(jnp.where(lane == 1, total, 0.0), axis=1, keepdims=True)
        return norm, curve

    norm_now = alpha = None
    for step in range(ITERS):
        operate()
        norm_next, curvature = two_products(step)
        if step == 0:
            ratio = None
            alpha = norm_next / curvature
        else:
            ratio = norm_next / norm_now
            alpha = norm_next / (curvature - ratio * norm_next / alpha)
        norm_now = norm_next

        def advance(i, carry, step=step, ratio=ratio, alpha=alpha):
            at = pl.multiple_of(i * 16, 8)
            here = pl.ds(pl.multiple_of(PAD + at, 8), 16)
            mine_rows = pl.ds(at, 16)
            way = res[here, 0:width]
            if step > 0:
                way = way + ratio * course[mine_rows, :]
            if step + 1 < ITERS:
                course[mine_rows, :] = way
            moved = alpha * way
            x_ref[mine_rows, :] = moved if step == 0 else x_ref[mine_rows, :] + moved
            if step + 1 == ITERS:
                r_ref[mine_rows, :] = res[here, 0:width] - alpha * (
                    image[here, 0:width] + ratio * along[here, 0:width]
                )
            return carry

        lax.fori_loop(0, height // 16, advance, 0)

        if step + 1 < ITERS:

            def recede(i, carry, step=step, ratio=ratio, alpha=alpha):
                here = pl.ds(start_of(i), STRIP)
                path = image[here, :]
                if step > 0:
                    path = path + ratio * along[here, :]
                along[here, :] = path
                res[here, :] = res[here, :] - alpha * path
                return carry

            lax.fori_loop(0, strips, recede, 0)


def per_device(rows, cols, obs_cell, obs_value, obs_weight, obs_count, kappa_field):
    count = rows * cols
    height, width = kappa_field.shape
    tiles, _, slots = obs_cell.shape[1:]
    cell = obs_cell[0]
    local = (cell // (width * cols) % TILE) * TILE + cell % TILE
    alive = jnp.arange(slots, dtype=jnp.int32) < obs_count[0][:, :, None]
    code = jnp.where(alive, local, -1).astype(jnp.int16).transpose(1, 0, 2)
    product = (obs_weight[0].astype(jnp.float32) * obs_value[0].astype(jnp.float32)).astype(jnp.bfloat16)
    pair = jnp.concatenate([obs_weight[0].transpose(1, 0, 2), product.transpose(1, 0, 2)], axis=1)

    in_vmem = pl.BlockSpec(memory_space=pltpu.VMEM)
    got_code, got_pair = pl.pallas_call(
        functools.partial(exchange_kernel, rows, cols),
        out_shape=(
            jax.ShapeDtypeStruct(code.shape, code.dtype),
            jax.ShapeDtypeStruct(pair.shape, pair.dtype),
        ),
        in_specs=[in_vmem] * 2,
        out_specs=(in_vmem,) * 2,
        scratch_shapes=[
            pltpu.SemaphoreType.DMA((2, count)),
            pltpu.SemaphoreType.DMA((2, count)),
            pltpu.SemaphoreType.DMA((2,)),
        ],
        compiler_params=pltpu.CompilerParams(collective_id=0, has_side_effects=True),
        name="exchange",
    )(code, pair)

    flat = got_code.astype(jnp.int32).transpose(1, 0, 2).reshape(tiles, 1, count * slots)
    pairs = (
        got_pair.reshape(count, 2, tiles, slots)
        .transpose(2, 1, 0, 3)
        .reshape(tiles, 2, count * slots)
        .astype(jnp.float32)
    )
    members = jnp.concatenate(
        [(flat >> 7).astype(jnp.float32), (flat & (TILE - 1)).astype(jnp.float32), pairs], axis=1
    )
    across = width // TILE
    field = jax.ShapeDtypeStruct((height, width), jnp.float32)
    tile_spec = pl.BlockSpec((TILE, TILE), lambda t: (t // across, t % across))
    weight_field, response = pl.pallas_call(
        bin_kernel,
        grid=(tiles,),
        out_shape=(field, field),
        in_specs=[pl.BlockSpec((1, 4, count * slots), lambda t: (t, 0, 0))],
        out_specs=(tile_spec, tile_spec),
        name="binning",
    )(members)

    full = width + 128
    tall = -(-(height + 2 * PAD) // 128) * 128
    extended = pltpu.VMEM((tall, full), jnp.float32)
    edge = pltpu.VMEM((3 * HALO, tall), jnp.float32)
    return pl.pallas_call(
        functools.partial(smooth_kernel, rows, cols),
        out_shape=(field, field),
        in_specs=[in_vmem] * 3,
        out_specs=(in_vmem,) * 2,
        scratch_shapes=[extended] * 7
        + [pltpu.VMEM((height, width), jnp.float32)]
        + [edge] * 4
        + [
            pltpu.VMEM((ITERS, 1, 128), jnp.float32),
            pltpu.VMEM((ITERS, count, 1, 128), jnp.float32),
            pltpu.SemaphoreType.DMA((2, 3)),
            pltpu.SemaphoreType.DMA((2, 3)),
            pltpu.SemaphoreType.DMA((2,)),
            pltpu.SemaphoreType.DMA((2,)),
            pltpu.SemaphoreType.DMA((ITERS, count)),
            pltpu.SemaphoreType.DMA((ITERS, count)),
        ],
        compiler_params=pltpu.CompilerParams(collective_id=1, has_side_effects=True),
        name="smoothing",
    )(response, weight_field, kappa_field)


def solution(mesh):
    placed = (
        P(("row", "col"), None, None, None),
        P(("row", "col"), None, None, None),
        P(("row", "col"), None, None, None),
        P(("row", "col"), None, None),
        P("row", "col"),
    )
    return jax.shard_map(
        functools.partial(per_device, mesh.shape["row"], mesh.shape["col"]),
        mesh=mesh,
        in_specs=placed,
        out_specs=(P("row", "col"), P("row", "col")),
        check_vma=False,
    )
```

```python
import functools

import jax
import jax.numpy as jnp
from jax import lax
from jax.experimental import pallas as pl
from jax.experimental.pallas import tpu as pltpu
from jax.sharding import PartitionSpec as P

TILE = 128
ITERS = 3
HALO = 8
PAD = 2 * HALO
STRIP = 88
CHUNK = 4096

smooth_weight = 0.05

MESH = pl.DeviceIdType.MESH


def greet_all(me, count, cols):
    barrier = pltpu.get_barrier_semaphore()

    def signal(k, carry):
        peer = lax.rem(me + k, count)
        pl.semaphore_signal(
            barrier, inc=1, device_id=(peer // cols, lax.rem(peer, cols)), device_id_type=MESH
        )
        return carry

    lax.fori_loop(1, count, signal, 0)


def await_all(count):
    pl.semaphore_wait(pltpu.get_barrier_semaphore(), count - 1)


def exchange_kernel(rows, cols, code_ref, pair_ref, code_out, pair_out, send_sems, recv_sems, own_sems):
    count = rows * cols
    me = lax.axis_index("row") * cols + lax.axis_index("col")
    own_code = pltpu.make_async_copy(code_ref.at[me], code_out.at[me], own_sems.at[0])
    own_pair = pltpu.make_async_copy(pair_ref.at[me], pair_out.at[me], own_sems.at[1])
    greet_all(me, count, cols)
    own_code.start()
    own_pair.start()
    await_all(count)

    def copies(k):
        peer = lax.rem(me + k, count)
        where = (peer // cols, lax.rem(peer, cols))
        return [
            pltpu.make_async_remote_copy(
                src_ref=src.at[peer],
                dst_ref=dst.at[me],
                send_sem=send_sems.at[which, k],
                recv_sem=recv_sems.at[which, k],
                device_id=where,
                device_id_type=MESH,
            )
            for which, (src, dst) in enumerate(((code_ref, code_out), (pair_ref, pair_out)))
        ]

    def begin(k, carry):
        for copy in copies(k):
            copy.start()
        return carry

    def finish(k, carry):
        source = lax.rem(me + count - k, count)
        for which, (src, dst) in enumerate(((code_ref, code_out), (pair_ref, pair_out))):
            pltpu.make_async_remote_copy(
                src_ref=src.at[source],
                dst_ref=dst.at[source],
                send_sem=send_sems.at[which, k],
                recv_sem=recv_sems.at[which, k],
                device_id=(source // cols, lax.rem(source, cols)),
                device_id_type=MESH,
            ).wait()
        return carry

    lax.fori_loop(1, count, begin, 0)
    lax.fori_loop(1, count, finish, 0)
    own_code.wait()
    own_pair.wait()


def bin_kernel(members_ref, weight_ref, response_ref):
    slots = members_ref.shape[2]
    chunk = min(CHUNK, slots)
    offsets = (
        lax.broadcasted_iota(jnp.int32, (TILE, chunk), 0).astype(jnp.float32).astype(jnp.bfloat16)
    )
    one = jnp.ones((TILE, chunk), jnp.bfloat16)
    zero = jnp.zeros((TILE, chunk), jnp.bfloat16)

    def part(at, total):
        def spread(which):
            piece = members_ref[0, which : which + 1, pl.ds(pl.multiple_of(at * chunk, chunk), chunk)]
            return jnp.broadcast_to(piece.astype(jnp.bfloat16), (TILE, chunk))

        col_hot = jnp.where(spread(1) == offsets, one, zero)
        row_hit = spread(0) == offsets
        stacked = jnp.concatenate(
            [jnp.where(row_hit, spread(2), zero), jnp.where(row_hit, spread(3), zero)], axis=0
        )
        return total + lax.dot_general(
            stacked, col_hot, (((1,), (1,)), ((), ())), preferred_element_type=jnp.float32
        )

    total = lax.fori_loop(
        0, slots // chunk, part, jnp.zeros((2 * TILE, TILE), jnp.float32)
    )
    weight_ref[...] = total[:TILE]
    response_ref[...] = total[TILE:]


def smooth_kernel(
    rows, cols, b_ref, w_ref, k_ref, x_ref, r_ref,
    res, wgt, kap, live, inner, image, along, second, further, course,
    send_low, send_high, recv_low, recv_high, mine, sums,
    row_send, row_recv, col_send, col_recv, sum_send, sum_recv,
):
    count = rows * cols
    my_row, my_col = lax.axis_index("row"), lax.axis_index("col")
    me = my_row * cols + my_col
    height, width = b_ref.shape
    full = width + 128
    own = pl.ds(PAD, height)
    fields = ((b_ref, res), (w_ref, wgt), (k_ref, kap))
    tall = res.shape[0]

    for _, field in fields:
        field[0:PAD, :] = jnp.zeros((PAD, full), jnp.float32)
        field[PAD + height :, :] = jnp.zeros((tall - PAD - height, full), jnp.float32)
    inner[0:HALO, :] = jnp.zeros((HALO, full), jnp.float32)
    inner[PAD + height + HALO : 2 * PAD + height, :] = jnp.zeros((HALO, full), jnp.float32)
    recv_low[...] = jnp.zeros_like(recv_low)
    recv_high[...] = jnp.zeros_like(recv_high)
    greet_all(me, count, cols)

    def fill(i, carry):
        at = pl.multiple_of(i * 32, 32)
        for src, dst in fields:
            dst[pl.ds(PAD + at, 32), 0:width] = src[pl.ds(at, 32), :]
        return carry

    lax.fori_loop(0, height // 32, fill, 0)

    await_all(count)

    up, down = my_row > 0, my_row < rows - 1
    left, right = my_col > 0, my_col < cols - 1

    def row_copies(way):
        made = []
        for at, (src, dst) in enumerate(fields):
            if way == 0:
                source, target = src.at[pl.ds(0, HALO), :], dst.at[pl.ds(PAD + height, HALO), pl.ds(0, width)]
                where = (my_row - 1, my_col)
            else:
                source, target = src.at[pl.ds(height - HALO, HALO), :], dst.at[pl.ds(HALO, HALO), pl.ds(0, width)]
                where = (my_row + 1, my_col)
            made.append(
                pltpu.make_async_remote_copy(
                    src_ref=source, dst_ref=target,
                    send_sem=row_send.at[way, at], recv_sem=row_recv.at[way, at],
                    device_id=where, device_id_type=MESH,
                )
            )
        return made

    def col_copy(way):
        source, target, where = (
            (send_low, recv_high, (my_row, my_col - 1)),
            (send_high, recv_low, (my_row, my_col + 1)),
        )[way]
        return pltpu.make_async_remote_copy(
            src_ref=source, dst_ref=target, send_sem=col_send.at[way], recv_sem=col_recv.at[way],
            device_id=where, device_id_type=MESH,
        )

    for way, there in ((0, up), (1, down)):

        @pl.when(there)
        def _(way=way):
            for copy in row_copies(way):
                copy.start()

    for way, there in ((0, up), (1, down)):

        @pl.when(there)
        def _(way=way):
            for copy in row_copies(way):
                copy.wait_send()

        @pl.when((down, up)[way])
        def _(way=way):
            for copy in row_copies(way):
                copy.wait_recv()

    def pack(i, carry):
        at = pl.multiple_of(i * 128, 128)
        for which, (_, field) in enumerate(fields):
            low = field[pl.ds(at, 128), 0:128].T
            send_low[which * HALO : (which + 1) * HALO, pl.ds(at, 128)] = low[:HALO]
            high = field[pl.ds(at, 128), width - 128 : width].T
            send_high[which * HALO : (which + 1) * HALO, pl.ds(at, 128)] = high[128 - HALO :]
        return carry

    lax.fori_loop(0, tall // 128, pack, 0)
    for way, there in ((0, left), (1, right)):

        @pl.when(there)
        def _(way=way):
            col_copy(way).start()

    for way, there in ((0, left), (1, right)):

        @pl.when(there)
        def _(way=way):
            col_copy(way).wait_send()

        @pl.when((right, left)[way])
        def _(way=way):
            col_copy(way).wait_recv()

    gap = jnp.zeros((128 - 2 * HALO, 128), jnp.float32)

    def unpack(i, carry):
        at = pl.multiple_of(i * 128, 128)
        for which, (_, field) in enumerate(fields):
            part = slice(which * HALO, (which + 1) * HALO)
            both = jnp.concatenate(
                [recv_high[part, pl.ds(at, 128)], gap, recv_low[part, pl.ds(at, 128)]], axis=0
            )
            field[pl.ds(at, 128), width:full] = both.T
        return carry

    lax.fori_loop(0, tall // 128, unpack, 0)

    strips = (height + 2 * HALO) // STRIP
    top = jnp.where(up, HALO, PAD)
    bottom = PAD + height + jnp.where(down, HALO, 0)
    high_end = width + jnp.where(right, HALO, 0)
    low_begin = full - jnp.where(left, HALO, 0)

    def start_of(i):
        return pl.multiple_of(HALO + i * STRIP, 8)

    def prepare(i, carry):
        at = start_of(i)
        row = lax.broadcasted_iota(jnp.int32, (STRIP, full), 0) + at
        col = lax.broadcasted_iota(jnp.int32, (STRIP, full), 1)
        inside = (row >= top) & (row < bottom) & ((col < high_end) | (col >= low_begin))
        mask = jnp.where(inside, 1.0, 0.0).astype(jnp.float32)
        live[pl.ds(at, STRIP), :] = mask
        kap[pl.ds(at, STRIP), :] = jnp.where(inside, 4.0 + kap[pl.ds(at, STRIP), :], 0.0)
        return carry

    lax.fori_loop(0, strips, prepare, 0)

    def stencil(field, at):
        slab = field[pl.ds(pl.multiple_of(at - HALO, 8), STRIP + 2 * HALO), :]
        center = slab[HALO : HALO + STRIP]
        beside = slab[HALO + 1 : HALO + 1 + STRIP] + slab[HALO - 1 : HALO - 1 + STRIP]
        beside = beside + pltpu.roll(center, full - 1, axis=1) + pltpu.roll(center, 1, axis=1)
        here = pl.ds(at, STRIP)
        return kap[here, :] * center - live[here, :] * beside

    def operate(source, target):
        def first(i, carry):
            at = start_of(i)
            inner[pl.ds(at, STRIP), :] = stencil(source, at)
            return carry

        def last(i, carry):
            at = start_of(i)
            here = pl.ds(at, STRIP)
            target[here, :] = wgt[here, :] * source[here, :] + smooth_weight * stencil(inner, at)
            return carry

        lax.fori_loop(0, strips, first, 0)
        lax.fori_loop(0, strips, last, 0)

    lane = lax.broadcasted_iota(jnp.int32, (1, 128), 1)

    def copy_to(step, k, peer, slot):
        return pltpu.make_async_remote_copy(
            src_ref=mine.at[step], dst_ref=sums.at[step, slot],
            send_sem=sum_send.at[step, k], recv_sem=sum_recv.at[step, k],
            device_id=(peer // cols, lax.rem(peer, cols)), device_id_type=MESH,
        )

    def begin_products(step):
        def add(i, carry):
            norm, curve = carry
            here = pl.ds(pl.multiple_of(PAD + i * 32, 8), 32)
            a, c = res[here, 0:width], image[here, 0:width]
            aa, ac = a * a, a * c
            norm = norm + ((aa[:8] + aa[8:16]) + (aa[16:24] + aa[24:]))
            return norm, curve + ((ac[:8] + ac[8:16]) + (ac[16:24] + ac[24:]))

        zero = jnp.zeros((8, width), jnp.float32)
        norm, curve = lax.fori_loop(0, height // 32, add, (zero, zero))
        norm = jnp.sum(jnp.sum(norm, axis=0, keepdims=True), axis=1, keepdims=True)
        curve = jnp.sum(jnp.sum(curve, axis=0, keepdims=True), axis=1, keepdims=True)
        both = jnp.where(lane == 0, norm, jnp.where(lane == 1, curve, 0.0))
        mine[step] = both
        sums[step, me] = both

        def begin(k, carry):
            copy_to(step, k, lax.rem(me + k, count), me).start()
            return carry

        lax.fori_loop(1, count, begin, 0)

    def end_products(step):
        def finish(k, carry):
            source = lax.rem(me + count - k, count)
            copy_to(step, k, source, source).wait()
            return carry

        lax.fori_loop(1, count, finish, 0)
        total = jnp.sum(sums[step], axis=0)
        norm = jnp.sum(jnp.where(lane == 0, total, 0.0), axis=1, keepdims=True)
        curve = jnp.sum(jnp.where(lane == 1, total, 0.0), axis=1, keepdims=True)
        return norm, curve

    operate(res, image)
    begin_products(0)
    norm_now = alpha = None
    for step in range(ITERS):
        if step + 1 < ITERS:
            operate(image, second)
        norm_next, curvature = end_products(step)
        if step == 0:
            ratio = None
            alpha = norm_next / curvature
        else:
            ratio = norm_next / norm_now
            alpha = norm_next / (curvature - ratio * norm_next / alpha)
        norm_now = norm_next

        if step + 1 < ITERS:

            def recede(i, carry, step=step, ratio=ratio, alpha=alpha):
                here = pl.ds(pl.multiple_of(HALO + i * 24, 8), 24)
                way, path, next_path = res[here, :], image[here, :], second[here, :]
                old, old_image = way, path
                if step > 0:
                    way = way + ratio * course[here, :]
                    path = path + ratio * along[here, :]
                    next_path = next_path + ratio * further[here, :]
                course[here, :] = way
                along[here, :] = path
                further[here, :] = next_path
                res[here, :] = old - alpha * path
                image[here, :] = old_image - alpha * next_path
                return carry

            lax.fori_loop(0, (height + 2 * HALO) // 24, recede, 0)
            begin_products(step + 1)

        def advance(i, carry, step=step, ratio=ratio, alpha=alpha):
            at = pl.multiple_of(i * 32, 32)
            here = pl.ds(pl.multiple_of(PAD + at, 8), 32)
            rows_here = pl.ds(at, 32)
            if step + 1 < ITERS:
                moved = alpha * course[here, 0:width]
            else:
                moved = alpha * (res[here, 0:width] + ratio * course[here, 0:width])
                r_ref[rows_here, :] = res[here, 0:width] - alpha * (
                    image[here, 0:width] + ratio * along[here, 0:width]
                )
            x_ref[rows_here, :] = moved if step == 0 else x_ref[rows_here, :] + moved
            return carry

        lax.fori_loop(0, height // 32, advance, 0)


def per_device(rows, cols, obs_cell, obs_value, obs_weight, obs_count, kappa_field):
    count = rows * cols
    height, width = kappa_field.shape
    tiles, _, slots = obs_cell.shape[1:]
    cell = obs_cell[0]
    local = (cell // (width * cols) % TILE) * TILE + cell % TILE
    alive = jnp.arange(slots, dtype=jnp.int32) < obs_count[0][:, :, None]
    code = jnp.where(alive, local, -1).astype(jnp.int16).transpose(1, 0, 2)
    product = (obs_weight[0].astype(jnp.float32) * obs_value[0].astype(jnp.float32)).astype(jnp.bfloat16)
    pair = jnp.concatenate([obs_weight[0].transpose(1, 0, 2), product.transpose(1, 0, 2)], axis=1)

    in_vmem = pl.BlockSpec(memory_space=pltpu.VMEM)
    got_code, got_pair = pl.pallas_call(
        functools.partial(exchange_kernel, rows, cols),
        out_shape=(
            jax.ShapeDtypeStruct(code.shape, code.dtype),
            jax.ShapeDtypeStruct(pair.shape, pair.dtype),
        ),
        in_specs=[in_vmem] * 2,
        out_specs=(in_vmem,) * 2,
        scratch_shapes=[
            pltpu.SemaphoreType.DMA((2, count)),
            pltpu.SemaphoreType.DMA((2, count)),
            pltpu.SemaphoreType.DMA((2,)),
        ],
        compiler_params=pltpu.CompilerParams(collective_id=0, has_side_effects=True, vmem_limit_bytes=8 << 20),
        name="exchange",
    )(code, pair)

    flat = got_code.astype(jnp.int32).transpose(1, 0, 2).reshape(tiles, 1, count * slots)
    pairs = (
        got_pair.reshape(count, 2, tiles, slots)
        .transpose(2, 1, 0, 3)
        .reshape(tiles, 2, count * slots)
        .astype(jnp.float32)
    )
    members = jnp.concatenate(
        [(flat >> 7).astype(jnp.float32), (flat & (TILE - 1)).astype(jnp.float32), pairs], axis=1
    )
    across = width // TILE
    field = jax.ShapeDtypeStruct((height, width), jnp.float32)
    tile_spec = pl.BlockSpec((TILE, TILE), lambda t: (t // across, t % across))
    weight_field, response = pl.pallas_call(
        bin_kernel,
        grid=(tiles,),
        out_shape=(field, field),
        in_specs=[pl.BlockSpec((1, 4, count * slots), lambda t: (t, 0, 0))],
        out_specs=(tile_spec, tile_spec),
        compiler_params=pltpu.CompilerParams(vmem_limit_bytes=24 << 20),
        name="binning",
    )(members)

    full = width + 128
    tall = -(-(height + 2 * PAD) // 128) * 128
    extended = pltpu.VMEM((tall, full), jnp.float32)
    edge = pltpu.VMEM((3 * HALO, tall), jnp.float32)
    return pl.pallas_call(
        functools.partial(smooth_kernel, rows, cols),
        out_shape=(field, field),
        in_specs=[in_vmem] * 3,
        out_specs=(in_vmem,) * 2,
        scratch_shapes=[extended] * 10
        + [edge] * 4
        + [
            pltpu.VMEM((ITERS, 1, 128), jnp.float32),
            pltpu.VMEM((ITERS, count, 1, 128), jnp.float32),
            pltpu.SemaphoreType.DMA((2, 3)),
            pltpu.SemaphoreType.DMA((2, 3)),
            pltpu.SemaphoreType.DMA((2,)),
            pltpu.SemaphoreType.DMA((2,)),
            pltpu.SemaphoreType.DMA((ITERS, count)),
            pltpu.SemaphoreType.DMA((ITERS, count)),
        ],
        compiler_params=pltpu.CompilerParams(collective_id=1, has_side_effects=True, vmem_limit_bytes=32 << 20),
        name="smoothing",
    )(response, weight_field, kappa_field)


def solution(mesh):
    placed = (
        P(("row", "col"), None, None, None),
        P(("row", "col"), None, None, None),
        P(("row", "col"), None, None, None),
        P(("row", "col"), None, None),
        P("row", "col"),
    )
    return jax.shard_map(
        functools.partial(per_device, mesh.shape["row"], mesh.shape["col"]),
        mesh=mesh,
        in_specs=placed,
        out_specs=(P("row", "col"), P("row", "col")),
        check_vma=False,
    )
```

```python
import functools

import jax
import jax.numpy as jnp
from jax import lax
from jax.experimental import pallas as pl
from jax.experimental.pallas import tpu as pltpu
from jax.sharding import PartitionSpec as P

TILE = 128
ITERS = 3
HALO = 8
PAD = 2 * HALO
STRIP = 176
SOURCES = 32
GROUP = 8

smooth_weight = 0.05

MESH = pl.DeviceIdType.MESH


def greet_all(me, count, cols):
    barrier = pltpu.get_barrier_semaphore()

    def signal(k, carry):
        peer = lax.rem(me + k, count)
        pl.semaphore_signal(
            barrier, inc=1, device_id=(peer // cols, lax.rem(peer, cols)), device_id_type=MESH
        )
        return carry

    lax.fori_loop(1, count, signal, 0)


def await_all(count):
    pl.semaphore_wait(pltpu.get_barrier_semaphore(), count - 1)


def observe_kernel(
    rows, cols, code_ref, pair_ref, weight_ref, response_ref,
    code_in, pair_in, place_row, place_col, amounts, send_sems, recv_sems, own_sems,
):
    count, groups, each, slots = code_ref.shape
    me = lax.axis_index("row") * cols + lax.axis_index("col")
    own_code = pltpu.make_async_copy(code_ref.at[me], code_in.at[me], own_sems.at[0])
    own_pair = pltpu.make_async_copy(pair_ref.at[me], pair_in.at[me], own_sems.at[1])
    greet_all(me, count, cols)
    own_code.start()
    own_pair.start()
    await_all(count)
    buffers = ((code_ref, code_in), (pair_ref, pair_in))

    def copies(group, k, peer, slot):
        return [
            pltpu.make_async_remote_copy(
                src_ref=src.at[peer, group],
                dst_ref=dst.at[slot, group],
                send_sem=send_sems.at[group, which, k],
                recv_sem=recv_sems.at[group, which, k],
                device_id=(peer // cols, lax.rem(peer, cols)),
                device_id_type=MESH,
            )
            for which, (src, dst) in enumerate(buffers)
        ]

    for group in range(groups):

        def begin(k, carry, group=group):
            for copy in copies(group, k, lax.rem(me + k, count), me):
                copy.start()
            return carry

        lax.fori_loop(1, count, begin, 0)
    own_code.wait()
    own_pair.wait()

    bunch = min(SOURCES, count)
    chunk = bunch * slots
    offsets = (
        lax.broadcasted_iota(jnp.int32, (TILE, chunk), 0).astype(jnp.float32).astype(jnp.bfloat16)
    )
    one = jnp.ones((TILE, chunk), jnp.bfloat16)
    zero = jnp.zeros((TILE, chunk), jnp.bfloat16)
    across = weight_ref.shape[1] // TILE

    for group in range(groups):

        def finish(k, carry, group=group):
            source = lax.rem(me + count - k, count)
            for copy in copies(group, k, source, source):
                copy.wait()
            return carry

        lax.fori_loop(1, count, finish, 0)

        def decode(i, carry, group=group):
            some = pl.ds(i * 8, 8)
            code = code_in[some, group].astype(jnp.int32).reshape(8 * each, slots)
            here = pl.ds(pl.multiple_of(i * 8 * each, 8 * each), 8 * each)
            place_row[here, :] = (code >> 7).astype(jnp.float32)
            place_col[here, :] = (code & (TILE - 1)).astype(jnp.float32)
            pair = pair_in[some, group].astype(jnp.float32).reshape(16 * each, slots)
            amounts[pl.ds(pl.multiple_of(i * 16 * each, 16 * each), 16 * each), :] = pair
            return carry

        lax.fori_loop(0, count // 8, decode, 0, unroll=2)

        def bin_tile(at, carry, group=group):
            def part(i, total):
                def spread(ref, first, step):
                    piece = ref[pl.ds(i * (bunch * step) + first, bunch, stride=step), :]
                    line = jnp.concatenate([piece[n : n + 1] for n in range(bunch)], axis=1)
                    return jnp.broadcast_to(line.astype(jnp.bfloat16), (TILE, chunk))

                col_hot = jnp.where(spread(place_col, at, each) == offsets, one, zero)
                row_hit = spread(place_row, at, each) == offsets
                weight = spread(amounts, at, 2 * each)
                product = spread(amounts, at + each, 2 * each)
                stacked = jnp.concatenate(
                    [jnp.where(row_hit, weight, zero), jnp.where(row_hit, product, zero)], axis=0
                )
                return total + lax.dot_general(
                    stacked, col_hot, (((1,), (1,)), ((), ())), preferred_element_type=jnp.float32
                )

            total = lax.fori_loop(
                0, count // bunch, part, jnp.zeros((2 * TILE, TILE), jnp.float32)
            )
            tile = group * each + at
            where = (
                pl.ds(pl.multiple_of((tile // across) * TILE, TILE), TILE),
                pl.ds(pl.multiple_of((tile % across) * TILE, TILE), TILE),
            )
            weight_ref[where] = total[:TILE]
            response_ref[where] = total[TILE:]
            return carry

        lax.fori_loop(0, each, bin_tile, 0, unroll=4)


def smooth_kernel(
    rows, cols, b_ref, w_ref, k_ref, x_ref, r_ref,
    res, wgt, kap, live, inner, image, along, second, further, course,
    send_low, send_high, recv_low, recv_high, mine, sums,
    row_send, row_recv, col_send, col_recv, sum_send, sum_recv,
):
    count = rows * cols
    my_row, my_col = lax.axis_index("row"), lax.axis_index("col")
    me = my_row * cols + my_col
    height, width = b_ref.shape
    full = width + 128
    own = pl.ds(PAD, height)
    fields = ((b_ref, res), (w_ref, wgt), (k_ref, kap))
    tall = res.shape[0]

    for _, field in fields:
        field[0:PAD, :] = jnp.zeros((PAD, full), jnp.float32)
        field[PAD + height :, :] = jnp.zeros((tall - PAD - height, full), jnp.float32)
    inner[0:HALO, :] = jnp.zeros((HALO, full), jnp.float32)
    inner[PAD + height + HALO : 2 * PAD + height, :] = jnp.zeros((HALO, full), jnp.float32)
    recv_low[...] = jnp.zeros_like(recv_low)
    recv_high[...] = jnp.zeros_like(recv_high)
    greet_all(me, count, cols)

    def fill(i, carry):
        at = pl.multiple_of(i * 32, 32)
        for src, dst in fields:
            dst[pl.ds(PAD + at, 32), 0:width] = src[pl.ds(at, 32), :]
        return carry

    lax.fori_loop(0, height // 32, fill, 0)

    await_all(count)

    up, down = my_row > 0, my_row < rows - 1
    left, right = my_col > 0, my_col < cols - 1

    def row_copies(way):
        made = []
        for at, (src, dst) in enumerate(fields):
            if way == 0:
                source, target = src.at[pl.ds(0, HALO), :], dst.at[pl.ds(PAD + height, HALO), pl.ds(0, width)]
                where = (my_row - 1, my_col)
            else:
                source, target = src.at[pl.ds(height - HALO, HALO), :], dst.at[pl.ds(HALO, HALO), pl.ds(0, width)]
                where = (my_row + 1, my_col)
            made.append(
                pltpu.make_async_remote_copy(
                    src_ref=source, dst_ref=target,
                    send_sem=row_send.at[way, at], recv_sem=row_recv.at[way, at],
                    device_id=where, device_id_type=MESH,
                )
            )
        return made

    def col_copy(way):
        source, target, where = (
            (send_low, recv_high, (my_row, my_col - 1)),
            (send_high, recv_low, (my_row, my_col + 1)),
        )[way]
        return pltpu.make_async_remote_copy(
            src_ref=source, dst_ref=target, send_sem=col_send.at[way], recv_sem=col_recv.at[way],
            device_id=where, device_id_type=MESH,
        )

    for way, there in ((0, up), (1, down)):

        @pl.when(there)
        def _(way=way):
            for copy in row_copies(way):
                copy.start()

    for way, there in ((0, up), (1, down)):

        @pl.when(there)
        def _(way=way):
            for copy in row_copies(way):
                copy.wait_send()

        @pl.when((down, up)[way])
        def _(way=way):
            for copy in row_copies(way):
                copy.wait_recv()

    def pack(i, carry):
        at = pl.multiple_of(i * 128, 128)
        for which, (_, field) in enumerate(fields):
            low = field[pl.ds(at, 128), 0:128].T
            send_low[which * HALO : (which + 1) * HALO, pl.ds(at, 128)] = low[:HALO]
            high = field[pl.ds(at, 128), width - 128 : width].T
            send_high[which * HALO : (which + 1) * HALO, pl.ds(at, 128)] = high[128 - HALO :]
        return carry

    lax.fori_loop(0, tall // 128, pack, 0, unroll=True)
    for way, there in ((0, left), (1, right)):

        @pl.when(there)
        def _(way=way):
            col_copy(way).start()

    for way, there in ((0, left), (1, right)):

        @pl.when(there)
        def _(way=way):
            col_copy(way).wait_send()

        @pl.when((right, left)[way])
        def _(way=way):
            col_copy(way).wait_recv()

    gap = jnp.zeros((128 - 2 * HALO, 128), jnp.float32)

    def unpack(i, carry):
        at = pl.multiple_of(i * 128, 128)
        for which, (_, field) in enumerate(fields):
            part = slice(which * HALO, (which + 1) * HALO)
            both = jnp.concatenate(
                [recv_high[part, pl.ds(at, 128)], gap, recv_low[part, pl.ds(at, 128)]], axis=0
            )
            field[pl.ds(at, 128), width:full] = both.T
        return carry

    lax.fori_loop(0, tall // 128, unpack, 0, unroll=True)

    strips = (height + 2 * HALO) // STRIP
    top = jnp.where(up, HALO, PAD)
    bottom = PAD + height + jnp.where(down, HALO, 0)
    high_end = width + jnp.where(right, HALO, 0)
    low_begin = full - jnp.where(left, HALO, 0)

    def start_of(i):
        return pl.multiple_of(HALO + i * STRIP, 8)

    def prepare(i, carry):
        at = start_of(i)
        row = lax.broadcasted_iota(jnp.int32, (STRIP, full), 0) + at
        col = lax.broadcasted_iota(jnp.int32, (STRIP, full), 1)
        inside = (row >= top) & (row < bottom) & ((col < high_end) | (col >= low_begin))
        mask = jnp.where(inside, 1.0, 0.0).astype(jnp.float32)
        live[pl.ds(at, STRIP), :] = mask
        kap[pl.ds(at, STRIP), :] = jnp.where(inside, 4.0 + kap[pl.ds(at, STRIP), :], 0.0)
        return carry

    lax.fori_loop(0, strips, prepare, 0)

    def stencil(field, at):
        slab = field[pl.ds(pl.multiple_of(at - HALO, 8), STRIP + 2 * HALO), :]
        center = slab[HALO : HALO + STRIP]
        beside = slab[HALO + 1 : HALO + 1 + STRIP] + slab[HALO - 1 : HALO - 1 + STRIP]
        beside = beside + pltpu.roll(center, full - 1, axis=1) + pltpu.roll(center, 1, axis=1)
        here = pl.ds(at, STRIP)
        return kap[here, :] * center - live[here, :] * beside

    def operate(source, target):
        def first(i, carry):
            at = start_of(i)
            inner[pl.ds(at, STRIP), :] = stencil(source, at)
            return carry

        def last(i, carry):
            at = start_of(i)
            here = pl.ds(at, STRIP)
            target[here, :] = wgt[here, :] * source[here, :] + smooth_weight * stencil(inner, at)
            return carry

        lax.fori_loop(0, strips, first, 0)
        lax.fori_loop(0, strips, last, 0)

    lane = lax.broadcasted_iota(jnp.int32, (1, 128), 1)

    def copy_to(step, k, peer, slot):
        return pltpu.make_async_remote_copy(
            src_ref=mine.at[step], dst_ref=sums.at[step, slot],
            send_sem=sum_send.at[step, k], recv_sem=sum_recv.at[step, k],
            device_id=(peer // cols, lax.rem(peer, cols)), device_id_type=MESH,
        )

    def begin_products(step):
        def add(i, carry):
            norm, curve = carry
            here = pl.ds(pl.multiple_of(PAD + i * 32, 8), 32)
            a, c = res[here, 0:width], image[here, 0:width]
            aa, ac = a * a, a * c
            norm = norm + ((aa[:8] + aa[8:16]) + (aa[16:24] + aa[24:]))
            return norm, curve + ((ac[:8] + ac[8:16]) + (ac[16:24] + ac[24:]))

        zero = jnp.zeros((8, width), jnp.float32)
        norm, curve = lax.fori_loop(0, height // 32, add, (zero, zero))
        norm = jnp.sum(jnp.sum(norm, axis=0, keepdims=True), axis=1, keepdims=True)
        curve = jnp.sum(jnp.sum(curve, axis=0, keepdims=True), axis=1, keepdims=True)
        both = jnp.where(lane == 0, norm, jnp.where(lane == 1, curve, 0.0))
        mine[step] = both
        sums[step, me] = both

        def begin(k, carry):
            copy_to(step, k, lax.rem(me + k, count), me).start()
            return carry

        lax.fori_loop(1, count, begin, 0, unroll=True)

    def end_products(step):
        def finish(k, carry):
            source = lax.rem(me + count - k, count)
            copy_to(step, k, source, source).wait()
            return carry

        lax.fori_loop(1, count, finish, 0, unroll=True)
        total = jnp.sum(sums[step], axis=0)
        norm = jnp.sum(jnp.where(lane == 0, total, 0.0), axis=1, keepdims=True)
        curve = jnp.sum(jnp.where(lane == 1, total, 0.0), axis=1, keepdims=True)
        return norm, curve

    operate(res, image)
    begin_products(0)
    norm_now = alpha = None
    for step in range(ITERS):
        if step + 1 < ITERS:
            operate(image, second)
        norm_next, curvature = end_products(step)
        if step == 0:
            ratio = None
            alpha = norm_next / curvature
        else:
            ratio = norm_next / norm_now
            alpha = norm_next / (curvature - ratio * norm_next / alpha)
        norm_now = norm_next

        if step + 1 < ITERS:

            def recede(i, carry, step=step, ratio=ratio, alpha=alpha):
                here = pl.ds(pl.multiple_of(HALO + i * 48, 8), 48)
                way, path, next_path = res[here, :], image[here, :], second[here, :]
                old, old_image = way, path
                if step > 0:
                    way = way + ratio * course[here, :]
                    path = path + ratio * along[here, :]
                    next_path = next_path + ratio * further[here, :]
                course[here, :] = way
                along[here, :] = path
                further[here, :] = next_path
                res[here, :] = old - alpha * path
                image[here, :] = old_image - alpha * next_path
                return carry

            lax.fori_loop(0, (height + 2 * HALO) // 48, recede, 0)
            begin_products(step + 1)

        def advance(i, carry, step=step, ratio=ratio, alpha=alpha):
            at = pl.multiple_of(i * 32, 32)
            here = pl.ds(pl.multiple_of(PAD + at, 8), 32)
            rows_here = pl.ds(at, 32)
            if step + 1 < ITERS:
                moved = alpha * course[here, 0:width]
            else:
                moved = alpha * (res[here, 0:width] + ratio * course[here, 0:width])
                r_ref[rows_here, :] = res[here, 0:width] - alpha * (
                    image[here, 0:width] + ratio * along[here, 0:width]
                )
            x_ref[rows_here, :] = moved if step == 0 else x_ref[rows_here, :] + moved
            return carry

        lax.fori_loop(0, height // 32, advance, 0)


def per_device(rows, cols, obs_cell, obs_value, obs_weight, obs_count, kappa_field):
    count = rows * cols
    height, width = kappa_field.shape
    tiles, _, slots = obs_cell.shape[1:]
    cell = obs_cell[0]
    local = (cell // (width * cols) % TILE) * TILE + cell % TILE
    alive = jnp.arange(slots, dtype=jnp.int32) < obs_count[0][:, :, None]
    code = jnp.where(alive, local, -1).astype(jnp.int16).transpose(1, 0, 2)
    product = (obs_weight[0].astype(jnp.float32) * obs_value[0].astype(jnp.float32)).astype(jnp.bfloat16)
    groups = tiles // GROUP
    code = code.reshape(count, groups, GROUP, slots)
    pair = jnp.concatenate(
        [
            array.transpose(1, 0, 2).reshape(count, groups, GROUP, slots)
            for array in (obs_weight[0], product)
        ],
        axis=2,
    )

    in_vmem = pl.BlockSpec(memory_space=pltpu.VMEM)
    field = jax.ShapeDtypeStruct((height, width), jnp.float32)
    weight_field, response = pl.pallas_call(
        functools.partial(observe_kernel, rows, cols),
        out_shape=(field, field),
        in_specs=[in_vmem] * 2,
        out_specs=(in_vmem,) * 2,
        scratch_shapes=[
            pltpu.VMEM(code.shape, code.dtype),
            pltpu.VMEM(pair.shape, pair.dtype),
            pltpu.VMEM((count * GROUP, slots), jnp.float32),
            pltpu.VMEM((count * GROUP, slots), jnp.float32),
            pltpu.VMEM((count * GROUP * 2, slots), jnp.float32),
            pltpu.SemaphoreType.DMA((groups, 2, count)),
            pltpu.SemaphoreType.DMA((groups, 2, count)),
            pltpu.SemaphoreType.DMA((2,)),
        ],
        compiler_params=pltpu.CompilerParams(
            collective_id=0, has_side_effects=True, vmem_limit_bytes=32 << 20
        ),
        name="observe",
    )(code, pair)

    full = width + 128
    tall = -(-(height + 2 * PAD) // 128) * 128
    extended = pltpu.VMEM((tall, full), jnp.float32)
    edge = pltpu.VMEM((3 * HALO, tall), jnp.float32)
    return pl.pallas_call(
        functools.partial(smooth_kernel, rows, cols),
        out_shape=(field, field),
        in_specs=[in_vmem] * 3,
        out_specs=(in_vmem,) * 2,
        scratch_shapes=[extended] * 10
        + [edge] * 4
        + [
            pltpu.VMEM((ITERS, 1, 128), jnp.float32),
            pltpu.VMEM((ITERS, count, 1, 128), jnp.float32),
            pltpu.SemaphoreType.DMA((2, 3)),
            pltpu.SemaphoreType.DMA((2, 3)),
            pltpu.SemaphoreType.DMA((2,)),
            pltpu.SemaphoreType.DMA((2,)),
            pltpu.SemaphoreType.DMA((ITERS, count)),
            pltpu.SemaphoreType.DMA((ITERS, count)),
        ],
        compiler_params=pltpu.CompilerParams(collective_id=1, has_side_effects=True, vmem_limit_bytes=32 << 20),
        name="smoothing",
    )(response, weight_field, kappa_field)


def solution(mesh):
    placed = (
        P(("row", "col"), None, None, None),
        P(("row", "col"), None, None, None),
        P(("row", "col"), None, None, None),
        P(("row", "col"), None, None),
        P("row", "col"),
    )
    return jax.shard_map(
        functools.partial(per_device, mesh.shape["row"], mesh.shape["col"]),
        mesh=mesh,
        in_specs=placed,
        out_specs=(P("row", "col"), P("row", "col")),
        check_vma=False,
    )
```
